32 devices in a mesh: box: 4 (over z), dir: 8 (over y, x, core).
Axes of the slice: x: 2, y: 2, z: 4, core: 2. Of those that a mesh axis runs over, the one named last changes fastest.
Arguments:
- currents: bfloat16 [4096, 256, 128], P(('box', 'dir')), may hold values from -6 to 6
- leaf_parent: int32 [4096], P(('box', 'dir')), may hold values from 0 to 63, as said below
- near_links: int32 [4096, 2], P(('box', 'dir')), may hold values 0 or 1
- near_blocks: bfloat16 [3, 256, 256], replicated, may hold values from -0.375 to 0.375
- aggregate_maps: bfloat16 [64, 256, 256], replicated, may hold values from -0.375 to 0.375
- far_boxes: int32 [64, 64], P('box'), may hold values from 0 to 63
- far_counts: int32 [64], P('box'), may hold values from 16 to 64
- translate_coef: float32 [64, 64, 256], P('box'), may hold values from 0.005 to 0.05
- time_kernel: float32 [128], replicated, may hold values from -0.5 to 0.5
- disaggregate_maps: bfloat16 [64, 256, 256], replicated, may hold values from -0.375 to 0.375
Outputs:
- field: bfloat16 [4096, 256, 128], P(('box', 'dir'))
The draws below stay inside these ranges and needn't reach their ends.
Inputs may be any that keep to these rules, and one draw needn't show every extreme that they name: `leaf_parent`: the leaves k * 64 to (k + 1) * 64 - 1 share one parent. The leaves g * 1024 to (g + 1) * 1024 - 1 have as parents the top-level boxes g * 16 to (g + 1) * 16 - 1, each exactly once as a run.
All inputs are finite; a program needn't handle non-finite values. No bound on the sum of `near_links` on one device may be relied on, other than what follows from the above.
Results may differ from the reference program's by a relative error of at most 0.0047.
Values may be sent and summed in bfloat16 or wider, within the bound.
A program may use at most 192 MiB of HBM per device.

```python
import math
import jax
import jax.numpy as jnp
from jax import lax

P_SIZE = 256
K_TOP = 256
S = 128
LEAF_TOP = 64
FAR = 64
LEAVES = 4096
GROUP_LEAVES = 1024
TOP_DEV = 16
TOPS = 64


def draw_leaf_parent(key, part):
    group_count = LEAVES // GROUP_LEAVES
    group_keys = jax.random.split(jax.random.fold_in(key, 11), group_count)
    orders = jax.vmap(lambda k: jax.random.permutation(k, TOP_DEV))(group_keys).astype(jnp.int32)
    leaf_index = jnp.arange(LEAVES, dtype=jnp.int32)
    group = leaf_index // GROUP_LEAVES
    run_index = leaf_index % GROUP_LEAVES // LEAF_TOP
    return (group * TOP_DEV + orders[group, run_index]).astype(jnp.int32)


def set_ends(entries, key, low, high):
    spot = [jax.random.randint(jax.random.fold_in(key, axis), (), 0, length) for axis, length in enumerate(entries.shape)]
    widest = entries.shape.index(max(entries.shape))
    beside = spot[:widest] + [(spot[widest] + 1) % entries.shape[widest]] + spot[widest + 1:]
    return entries.at[tuple(spot)].set(low).at[tuple(beside)].set(high)


def level_of(stream_key, shape, shards, smallest, top_value):
    def one(axis_at, shards_of):
        draws = jax.random.uniform(jax.random.fold_in(jax.random.fold_in(stream_key, 6), axis_at), (shards_of,), jnp.float32, smallest / len(shards), top_value / len(shards))
        return jnp.repeat(jnp.exp(draws), shape[axis_at] // shards_of).reshape((-1,) + (1,) * (len(shape) - axis_at - 1))

    level = one(*shards[0])
    for cut in shards[1:]:
        level = level * one(*cut)
    return level


def bell_draw(own_key, dims, deviation, bound, cuts=(), kind=jnp.bfloat16):
    values = deviation * jax.random.normal(own_key, dims, jnp.float32)
    if cuts:
        values = values * level_of(own_key, dims, cuts, -0.22, 0.18)
    return jnp.clip(values, -bound, bound).astype(kind)


def setup_inputs(seed: int = 0) -> dict:
    key_of = jax.random.split(jax.random.key(seed), 11)
    currents = bell_draw(key_of[0], (LEAVES, P_SIZE, S), 1.0, 6.0, ((0, 32),))
    leaf_parent = draw_leaf_parent(jax.random.fold_in(key_of[10], 71), 0)
    near_links = set_ends((jax.random.randint(key_of[2], (LEAVES, 2), 0, 4) < 3).astype(jnp.int32), jax.random.fold_in(key_of[2], 1), 0, 1)
    near_blocks = bell_draw(key_of[3], (3, P_SIZE, P_SIZE), P_SIZE ** -0.5, 0.375)
    aggregate_maps = bell_draw(key_of[4], (LEAF_TOP, K_TOP, P_SIZE), P_SIZE ** -0.5, 0.375)
    far_boxes = set_ends(jax.random.randint(key_of[5], (TOPS, FAR), 0, TOPS), jax.random.fold_in(key_of[5], 1), 0, TOPS - 1).astype(jnp.int32)
    far_counts = set_ends(jax.random.randint(key_of[6], (TOPS,), FAR // 4, FAR + 1), jax.random.fold_in(key_of[6], 1), FAR // 4, FAR).astype(jnp.int32)
    translate_coef = jnp.clip(jnp.exp(math.log(0.05) - 2.3025851 * jax.random.uniform(key_of[7], (TOPS, FAR, K_TOP), jnp.float32) ** level_of(key_of[7], (TOPS, FAR, K_TOP), ((0, 4),), -0.2, 0.2)), 0.005, 0.05)
    time_kernel = bell_draw(key_of[8], (S,), S ** -0.5, 0.5, (), jnp.float32)
    disaggregate_maps = bell_draw(key_of[9], (LEAF_TOP, P_SIZE, K_TOP), K_TOP ** -0.5, 0.375)
    return dict(currents=currents, leaf_parent=leaf_parent, near_links=near_links, near_blocks=near_blocks, aggregate_maps=aggregate_maps, far_boxes=far_boxes, far_counts=far_counts, translate_coef=translate_coef, time_kernel=time_kernel, disaggregate_maps=disaggregate_maps)


def time_matrix(kernel):
    sample_lag = jnp.arange(S)[:, None] - jnp.arange(S)[None, :]
    return jnp.where(sample_lag >= 0, kernel[jnp.clip(sample_lag, 0, S - 1)], jnp.zeros((), kernel.dtype))


def reference(currents, leaf_parent, near_links, near_blocks, aggregate_maps, far_boxes, far_counts, translate_coef, time_kernel, disaggregate_maps):
    highest = lax.Precision.HIGHEST
    blocks = LEAVES // 8
    agg_float = aggregate_maps.astype(jnp.float32)
    cur_blocks = currents.reshape(blocks, 8, P_SIZE, S)
    par_blocks = leaf_parent.reshape(blocks, 8)
    block_ids = jnp.arange(blocks, dtype=jnp.int32)

    def add_block(running, inputs):
        block_cur, block_par, block_id = inputs
        first_map = ((block_id * 8) % LEAF_TOP).astype(jnp.int32)
        map_block = lax.dynamic_slice_in_dim(agg_float, first_map, 8, 0)
        ray_terms = jnp.einsum('sqp,spt->sqt', map_block, block_cur.astype(jnp.float32), precision=highest)
        return running.at[block_par].add(ray_terms), None

    top_rays, _ = lax.scan(add_block, jnp.zeros((TOPS, K_TOP, S), jnp.float32), (cur_blocks, par_blocks, block_ids))
    top_rays = top_rays.astype(jnp.bfloat16)
    is_valid = (jnp.arange(FAR)[None, :] < far_counts[:, None]).astype(jnp.float32)
    matches = (far_boxes[:, :, None] == jnp.arange(TOPS)[None, None, :]).astype(jnp.float32) * is_valid[:, :, None]
    weights = jnp.einsum('cfs,cfq->csq', matches, translate_coef, precision=highest)
    far_sum = jnp.einsum('csq,sqt->cqt', weights, top_rays.astype(jnp.float32), precision=highest)
    incoming = jnp.einsum('cqs,ts->cqt', far_sum, time_matrix(time_kernel), precision=highest).astype(jnp.bfloat16)
    incoming_float = incoming.astype(jnp.float32)
    zero_leaf = jnp.zeros((1, P_SIZE, S), currents.dtype)
    padded = jnp.concatenate([zero_leaf, currents, zero_leaf], axis=0)
    near_float = near_blocks.astype(jnp.float32)
    dis_float = disaggregate_maps.astype(jnp.float32)

    def leaf_block(block_index):
        first_leaf = (block_index * 8).astype(jnp.int32)
        first_map = (first_leaf % LEAF_TOP).astype(jnp.int32)
        before_leaf = lax.dynamic_slice_in_dim(padded, first_leaf, 8, 0).astype(jnp.float32)
        middle_leaf = lax.dynamic_slice_in_dim(padded, first_leaf + 1, 8, 0).astype(jnp.float32)
        after_leaf = lax.dynamic_slice_in_dim(padded, first_leaf + 2, 8, 0).astype(jnp.float32)
        link_mask = lax.dynamic_slice_in_dim(near_links, first_leaf, 8, 0).astype(jnp.float32)
        parents = lax.dynamic_slice_in_dim(leaf_parent, first_leaf, 8, 0)
        map_block = lax.dynamic_slice_in_dim(dis_float, first_map, 8, 0)
        near_field = jnp.einsum('pr,srt->spt', near_float[0], middle_leaf, precision=highest)
        near_field = near_field + link_mask[:, 0, None, None] * jnp.einsum('pr,srt->spt', near_float[1], before_leaf, precision=highest)
        near_field = near_field + link_mask[:, 1, None, None] * jnp.einsum('pr,srt->spt', near_float[2], after_leaf, precision=highest)
        far_field = jnp.einsum('spq,sqt->spt', map_block, incoming_float[parents], precision=highest)
        return (near_field + far_field).astype(jnp.bfloat16)

    field_out = lax.map(leaf_block, jnp.arange(blocks, dtype=jnp.int32))
    return field_out.reshape(LEAVES, P_SIZE, S)
```

```python
import functools
import jax
import jax.numpy as jnp
from jax import lax
from jax.experimental import pallas as pl
from jax.experimental.pallas import tpu as pltpu
from jax.sharding import PartitionSpec as P

LEAF_TOP = 64
MESH = pl.DeviceIdType.MESH
HIGHEST = lax.Precision.HIGHEST


def aggregate_kernel(runs, chunk, maps_ref, cur_ref, out_ref, acc_ref):
    step = pl.program_id(0)
    samples = cur_ref.shape[-1]

    @pl.when(step == 0)
    def _():
        acc_ref[...] = jnp.zeros_like(acc_ref)

    total = acc_ref[...]
    for i in range(chunk):
        pair = jnp.concatenate([cur_ref[j, i] for j in range(runs)], axis=1)
        total = total + jnp.dot(maps_ref[i], pair, preferred_element_type=jnp.float32)
    acc_ref[...] = total

    @pl.when(step == pl.num_programs(0) - 1)
    def _():
        for j in range(runs):
            out_ref[j] = acc_ref[:, j * samples : (j + 1) * samples].astype(jnp.bfloat16)


def translate_kernel(
    boxes,
    dirs,
    runs,
    top_local,
    rays_ref,
    parent_ref,
    lists_ref,
    coef_ref,
    kernel_ref,
    out_ref,
    rays_all,
    parent_all,
    weights_ref,
    far_ref,
    stage_ref,
    landed,
    ray_send,
    ray_recv,
    par_send,
    par_recv,
    back_send,
    back_recv,
):
    my_box = lax.axis_index("box")
    my_dir = lax.axis_index("dir")
    me = my_box * dirs + my_dir
    rows = coef_ref.shape[1]
    samples = rays_ref.shape[-1]
    peers = [(kb, kd) for kb in range(boxes) for kd in range(dirs) if kb or kd]
    peers.sort(key=lambda p: -min(p[0], boxes - p[0]))

    def target(kb, kd):
        return lax.rem(my_box + kb, boxes), lax.rem(my_dir + kd, dirs)

    barrier = pltpu.get_barrier_semaphore()
    for kb, kd in peers:
        tb, td = target(kb, kd)
        pl.semaphore_signal(
            barrier, inc=1, device_id={"box": tb, "dir": td}, device_id_type=MESH
        )
    pl.semaphore_wait(barrier, len(peers))

    def parent_copy(kb, kd):
        tb, td = target(kb, kd)
        return pltpu.make_async_remote_copy(
            src_ref=parent_ref,
            dst_ref=parent_all.at[me],
            send_sem=par_send.at[tb * dirs + td],
            recv_sem=par_recv.at[me],
            device_id={"box": tb, "dir": td},
            device_id_type=MESH,
        )

    def ray_copy(kb, kd):
        tb, td = target(kb, kd)
        block = pl.ds(pl.multiple_of(td * rows, rows), rows)
        return pltpu.make_async_remote_copy(
            src_ref=rays_ref.at[:, block, :],
            dst_ref=rays_all.at[me],
            send_sem=ray_send.at[tb * dirs + td],
            recv_sem=ray_recv.at[me],
            device_id={"box": tb, "dir": td},
            device_id_type=MESH,
        )

    for kb, kd in peers:
        parent_copy(kb, kd).start()
    for kb, kd in peers:
        ray_copy(kb, kd).start()

    own = pl.ds(pl.multiple_of(my_dir * rows, rows), rows)
    rays_all[me] = rays_ref[:, own, :]
    parent_all[me] = parent_ref[...]

    lag = lax.broadcasted_iota(jnp.int32, (samples, samples), 1) - lax.broadcasted_iota(
        jnp.int32, (samples, samples), 0
    )

    def add_lag(i, matrix):
        return jnp.where(lag == i, kernel_ref[i], matrix)

    time_matrix = lax.fori_loop(
        0, samples, add_lag, jnp.zeros((samples, samples), jnp.float32)
    )

    def arrived(slot, buffer, sem):
        pltpu.make_async_remote_copy(
            src_ref=buffer.at[slot],
            dst_ref=buffer.at[slot],
            send_sem=sem.at[slot],
            recv_sem=sem.at[slot],
            device_id={"box": my_box, "dir": lax.rem(my_dir + 1, dirs)},
            device_id_type=MESH,
        ).wait_recv()

    for kb, kd in peers:
        sb, sd = target(kb, kd)
        arrived(sb * dirs + sd, parent_all, par_recv)
    parents = jnp.zeros((1, parent_ref.shape[-1]), jnp.float32)
    for slot in range(boxes * dirs):
        parents = parents + parent_all[slot]
    for c in range(top_local):
        match = (lists_ref[:, c : c + 1] == parents).astype(jnp.float32)
        weights_ref[c] = jnp.dot(
            coef_ref[c], match, preferred_element_type=jnp.float32, precision=HIGHEST
        )

    for kb, kd in peers:
        sb, sd = target(kb, kd)
        arrived(sb * dirs + sd, rays_all, ray_recv)

    group = 4 if top_local % 4 == 0 else 1

    def far_group(g, carry):
        base = g * group
        weight = [weights_ref[base + i] for i in range(group)]
        total = [jnp.zeros((rows, samples), jnp.float32) for _ in range(group)]
        for slot in range(boxes * dirs):
            for j in range(runs):
                ray = rays_all[slot, j].astype(jnp.float32)
                at = slot * runs + j
                for i in range(group):
                    total[i] = total[i] + weight[i][:, at : at + 1] * ray
        for i in range(group):
            far_ref[base + i] = total[i]
        return carry

    lax.fori_loop(0, top_local // group, far_group, 0)

    incoming = jnp.dot(
        far_ref[...].reshape(top_local * rows, samples),
        time_matrix,
        preferred_element_type=jnp.float32,
        precision=HIGHEST,
    )
    far_ref[...] = incoming.reshape(top_local, rows, samples)
    first_top = my_box * top_local
    for d in range(dirs):
        held = parent_all[my_box * dirs + d]
        for j in range(runs):
            lane = lax.broadcasted_iota(jnp.int32, held.shape, 1)
            at = (my_box * dirs + d) * runs + j
            parent = jnp.sum(jnp.where(lane == at, held, 0.0), axis=1, keepdims=True)
            chosen = jnp.zeros((rows, samples), jnp.float32)
            for c in range(top_local):
                hit = parent == (first_top + c).astype(jnp.float32)
                chosen = jnp.where(hit, far_ref[c], chosen)
            stage_ref[d, j] = chosen.astype(jnp.bfloat16)

    def back_copy(kd):
        td = lax.rem(my_dir + kd, dirs)
        return pltpu.make_async_remote_copy(
            src_ref=stage_ref.at[td],
            dst_ref=landed.at[my_dir],
            send_sem=back_send.at[td],
            recv_sem=back_recv.at[my_dir],
            device_id={"box": my_box, "dir": td},
            device_id_type=MESH,
        )

    for kd in range(1, dirs):
        back_copy(kd).start()
    landed[my_dir] = stage_ref[my_dir]
    for kb, kd in peers:
        parent_copy(kb, kd).wait_send()
        ray_copy(kb, kd).wait_send()
    for kd in range(1, dirs):
        sd = lax.rem(my_dir + kd, dirs)
        arrived(sd, landed, back_recv)
    for d in range(dirs):
        for j in range(runs):
            out_ref[d * rows : (d + 1) * rows, j * samples : (j + 1) * samples] = landed[d, j]
    for kd in range(1, dirs):
        back_copy(kd).wait_send()


def field_kernel(
    runs,
    chunk,
    blocks_ref,
    maps_ref,
    incoming_ref,
    mask_ref,
    cur_ref,
    before_ref,
    after_ref,
    first_ref,
    last_ref,
    out_ref,
):
    step = pl.program_id(0)
    samples = cur_ref.shape[-1]

    def joined(parts):
        return jnp.concatenate(parts, axis=1)

    lead = joined([jnp.where(step == 0, first_ref[j], before_ref[j, 0]) for j in range(runs)])
    final = step == pl.num_programs(0) - 1
    tail = joined([jnp.where(final, last_ref[j], after_ref[j, 0]) for j in range(runs)])
    pairs = [lead]
    pairs += [joined([cur_ref[j, i] for j in range(runs)]) for i in range(chunk)]
    pairs += [tail]
    dot = functools.partial(jnp.dot, preferred_element_type=jnp.float32)
    for i in range(chunk):
        total = dot(blocks_ref[0], pairs[i + 1]) + dot(maps_ref[i], incoming_ref[...])
        total = total + mask_ref[0, i] * dot(blocks_ref[1], pairs[i])
        total = total + mask_ref[1, i] * dot(blocks_ref[2], pairs[i + 2])
        for j in range(runs):
            out_ref[j, i] = total[:, j * samples : (j + 1) * samples].astype(jnp.bfloat16)


def per_device(
    currents,
    leaf_parent,
    near_links,
    near_blocks,
    aggregate_maps,
    far_boxes,
    far_counts,
    translate_coef,
    time_kernel,
    disaggregate_maps,
):
    boxes, dirs = lax.axis_size("box"), lax.axis_size("dir")
    devices = boxes * dirs
    leaf_count, unknowns, samples = currents.shape
    runs = leaf_count // LEAF_TOP
    top_local, list_slots = far_boxes.shape
    directions = aggregate_maps.shape[1]
    rows = directions // dirs
    box_index, dir_index = lax.axis_index("box"), lax.axis_index("dir")
    me = box_index * dirs + dir_index
    f32, bf16 = jnp.float32, jnp.bfloat16

    chain = [(i, i + 1) for i in range(devices - 1)]
    low = lax.ppermute(currents[-1:], ("box", "dir"), chain)
    high = lax.ppermute(currents[:1], ("box", "dir"), [(b, a) for a, b in chain])
    leaf_runs = currents.reshape(runs, LEAF_TOP, unknowns, samples)

    chunk = 8
    steps = LEAF_TOP // chunk
    matmul_cost = 2 * leaf_count * samples * unknowns * directions
    vmem = pl.BlockSpec(memory_space=pltpu.VMEM)
    rays = pl.pallas_call(
        functools.partial(aggregate_kernel, runs, chunk),
        out_shape=jax.ShapeDtypeStruct((runs, directions, samples), bf16),
        grid=(steps,),
        in_specs=[
            pl.BlockSpec((chunk, directions, unknowns), lambda i: (i, 0, 0)),
            pl.BlockSpec((runs, chunk, unknowns, samples), lambda i: (0, i, 0, 0)),
        ],
        out_specs=pl.BlockSpec((runs, directions, samples), lambda i: (0, 0, 0)),
        scratch_shapes=[pltpu.VMEM((directions, runs * samples), f32)],
        cost_estimate=pl.CostEstimate(
            flops=matmul_cost, bytes_accessed=16 * 2**20, transcendentals=0
        ),
        name="aggregate",
    )(aggregate_maps, leaf_runs)

    total_runs = devices * runs
    width = -(-total_runs // 128) * 128
    run_parent = leaf_parent.reshape(runs, LEAF_TOP)[:, 0].astype(f32)
    lane = jnp.arange(width)
    parent_row = jnp.sum(
        jnp.where(
            lane[None, :] == (me * runs + jnp.arange(runs))[:, None], run_parent[:, None], 0.0
        ),
        axis=0,
    )
    parent_row = jnp.where((lane >= total_runs) & (me == 0), -2.0, parent_row)[None, :]
    is_valid = jnp.arange(list_slots)[None, :] < far_counts[:, None]
    lists = jnp.where(is_valid, far_boxes, -1).astype(f32).T
    coef = lax.dynamic_slice_in_dim(translate_coef, dir_index * rows, rows, 2).transpose(0, 2, 1)
    dma = pltpu.SemaphoreType.DMA
    incoming = pl.pallas_call(
        functools.partial(translate_kernel, boxes, dirs, runs, top_local),
        out_shape=jax.ShapeDtypeStruct((directions, runs * samples), bf16),
        in_specs=[vmem, vmem, vmem, vmem, pl.BlockSpec(memory_space=pltpu.SMEM)],
        out_specs=vmem,
        scratch_shapes=[
            pltpu.VMEM((devices, runs, rows, samples), bf16),
            pltpu.VMEM((devices, 1, width), f32),
            pltpu.VMEM((top_local, rows, width), f32),
            pltpu.VMEM((top_local, rows, samples), f32),
            pltpu.VMEM((dirs, runs, rows, samples), bf16),
            pltpu.VMEM((dirs, runs, rows, samples), bf16),
            dma((devices,)),
            dma((devices,)),
            dma((devices,)),
            dma((devices,)),
            dma((dirs,)),
            dma((dirs,)),
        ],
        compiler_params=pltpu.CompilerParams(collective_id=0, has_side_effects=True),
        name="translate",
    )(rays, parent_row, lists, coef, time_kernel)

    first = jnp.concatenate([low, currents[LEAF_TOP - 1 : -1 : LEAF_TOP]], axis=0)
    last = jnp.concatenate([currents[LEAF_TOP::LEAF_TOP], high], axis=0)
    mask = near_links.astype(f32).reshape(runs, LEAF_TOP, 2).transpose(2, 1, 0)
    mask = jnp.repeat(mask, samples, axis=2)[:, :, None, :]
    near_cost = 4 * matmul_cost
    out = pl.pallas_call(
        functools.partial(field_kernel, runs, chunk),
        out_shape=jax.ShapeDtypeStruct((runs, LEAF_TOP, unknowns, samples), bf16),
        grid=(steps,),
        in_specs=[
            vmem,
            pl.BlockSpec((chunk, unknowns, directions), lambda i: (i, 0, 0)),
            vmem,
            pl.BlockSpec((2, chunk, 1, runs * samples), lambda i: (0, i, 0, 0)),
            pl.BlockSpec((runs, chunk, unknowns, samples), lambda i: (0, i, 0, 0)),
            pl.BlockSpec(
                (runs, 1, unknowns, samples), lambda i: (0, jnp.maximum(i * chunk - 1, 0), 0, 0)
            ),
            pl.BlockSpec(
                (runs, 1, unknowns, samples),
                lambda i: (0, jnp.minimum((i + 1) * chunk, LEAF_TOP - 1), 0, 0),
            ),
            vmem,
            vmem,
        ],
        out_specs=pl.BlockSpec((runs, chunk, unknowns, samples), lambda i: (0, i, 0, 0)),
        cost_estimate=pl.CostEstimate(
            flops=near_cost, bytes_accessed=26 * 2**20, transcendentals=0
        ),
        name="field",
    )(near_blocks, disaggregate_maps, incoming, mask, leaf_runs, leaf_runs, leaf_runs, first, last)
    return out.reshape(leaf_count, unknowns, samples)


def solution(mesh):
    return jax.shard_map(
        per_device,
        mesh=mesh,
        in_specs=(
            P(("box", "dir"), None, None),
            P(("box", "dir")),
            P(("box", "dir"), None),
            P(),
            P(),
            P("box", None),
            P("box"),
            P("box", None, None),
            P(),
            P(),
        ),
        out_specs=P(("box", "dir"), None, None),
        check_vma=False,
    )
```

```python
import functools
import jax
import jax.numpy as jnp
from jax import lax
from jax.experimental import pallas as pl
from jax.experimental.pallas import tpu as pltpu
from jax.sharding import PartitionSpec as P

LEAF_TOP = 64
MESH = pl.DeviceIdType.MESH
HIGHEST = lax.Precision.HIGHEST


def aggregate_kernel(runs, chunk, maps_ref, cur_ref, out_ref, acc_ref):
    step = pl.program_id(0)
    samples = cur_ref.shape[-1]

    @pl.when(step == 0)
    def _():
        acc_ref[...] = jnp.zeros_like(acc_ref)

    total = acc_ref[...]
    for i in range(chunk):
        pair = jnp.concatenate([cur_ref[j, i] for j in range(runs)], axis=1)
        total = total + jnp.dot(maps_ref[i], pair, preferred_element_type=jnp.float32)
    acc_ref[...] = total

    @pl.when(step == pl.num_programs(0) - 1)
    def _():
        for j in range(runs):
            out_ref[j] = acc_ref[:, j * samples : (j + 1) * samples].astype(jnp.bfloat16)


def translate_kernel(
    boxes,
    dirs,
    runs,
    top_local,
    rays_ref,
    edge_ref,
    leaf_parent_ref,
    lists_ref,
    counts_ref,
    coef_ref,
    kernel_ref,
    out_ref,
    rim_ref,
    parent_ref,
    rim,
    rays_all,
    parent_all,
    weights_ref,
    far_ref,
    stage_ref,
    landed,
    ray_send,
    ray_recv,
    par_send,
    par_recv,
    back_send,
    back_recv,
    rim_send,
    rim_recv,
):
    my_box = lax.axis_index("box")
    my_dir = lax.axis_index("dir")
    me = my_box * dirs + my_dir
    devices = boxes * dirs
    rows = coef_ref.shape[2]
    samples = rays_ref.shape[-1]
    width = parent_ref.shape[-1]
    lane = lax.broadcasted_iota(jnp.int32, (1, width), 1)
    spare = jnp.where(me == 0, -1, 0)
    parent_row = jnp.where(lane >= devices * runs, spare, jnp.zeros((1, width), jnp.int32))
    for j in range(runs):
        parent_row = jnp.where(lane == me * runs + j, leaf_parent_ref[j * LEAF_TOP], parent_row)
    parent_ref[...] = parent_row.astype(jnp.float32)
    rim[...] = jnp.zeros_like(rim)
    peers = [(kb, kd) for kb in range(boxes) for kd in range(dirs) if kb or kd]
    peers.sort(key=lambda p: -min(p[0], boxes - p[0]))

    def target(kb, kd):
        return lax.rem(my_box + kb, boxes), lax.rem(my_dir + kd, dirs)

    barrier = pltpu.get_barrier_semaphore()
    for kb, kd in peers:
        tb, td = target(kb, kd)
        pl.semaphore_signal(
            barrier, inc=1, device_id={"box": tb, "dir": td}, device_id_type=MESH
        )
    pl.semaphore_wait(barrier, len(peers))

    def parent_copy(kb, kd):
        tb, td = target(kb, kd)
        return pltpu.make_async_remote_copy(
            src_ref=parent_ref,
            dst_ref=parent_all.at[me],
            send_sem=par_send.at[tb * dirs + td],
            recv_sem=par_recv.at[me],
            device_id={"box": tb, "dir": td},
            device_id_type=MESH,
        )

    def ray_copy(kb, kd):
        tb, td = target(kb, kd)
        block = pl.ds(pl.multiple_of(td * rows, rows), rows)
        return pltpu.make_async_remote_copy(
            src_ref=rays_ref.at[:, block, :],
            dst_ref=rays_all.at[me],
            send_sem=ray_send.at[tb * dirs + td],
            recv_sem=ray_recv.at[me],
            device_id={"box": tb, "dir": td},
            device_id_type=MESH,
        )

    def rim_copy(side):
        other = lax.rem(me + (1 if side == 0 else devices - 1), devices)
        return pltpu.make_async_remote_copy(
            src_ref=edge_ref.at[side],
            dst_ref=rim.at[side],
            send_sem=rim_send.at[side],
            recv_sem=rim_recv.at[side],
            device_id={"box": lax.div(other, dirs), "dir": lax.rem(other, dirs)},
            device_id_type=MESH,
        )

    for kb, kd in peers:
        parent_copy(kb, kd).start()
    for kb, kd in peers:
        ray_copy(kb, kd).start()

    @pl.when(me < devices - 1)
    def _():
        rim_copy(0).start()

    @pl.when(me > 0)
    def _():
        rim_copy(1).start()

    own = pl.ds(pl.multiple_of(my_dir * rows, rows), rows)
    rays_all[me] = rays_ref[:, own, :]
    parent_all[me] = parent_ref[...]

    lag = lax.broadcasted_iota(jnp.int32, (samples, samples), 1) - lax.broadcasted_iota(
        jnp.int32, (samples, samples), 0
    )

    def add_lag(i, matrix):
        return jnp.where(lag == i, kernel_ref[i], matrix)

    time_matrix = lax.fori_loop(
        0, samples, add_lag, jnp.zeros((samples, samples), jnp.float32)
    )

    def arrived(slot, buffer, sem):
        pltpu.make_async_remote_copy(
            src_ref=buffer.at[slot],
            dst_ref=buffer.at[slot],
            send_sem=sem.at[slot],
            recv_sem=sem.at[slot],
            device_id={"box": my_box, "dir": lax.rem(my_dir + 1, dirs)},
            device_id_type=MESH,
        ).wait_recv()

    for kb, kd in peers:
        sb, sd = target(kb, kd)
        arrived(sb * dirs + sd, parent_all, par_recv)
    parents = jnp.zeros((1, width), jnp.float32)
    for slot in range(devices):
        parents = parents + parent_all[slot]
    slots = lists_ref.shape[1]
    column = jnp.broadcast_to(parents, (128, width)).T[:, :slots]
    spot = lax.broadcasted_iota(jnp.int32, (1, slots), 1)
    for c in range(top_local):
        used = jnp.where(spot < counts_ref[c], lists_ref[c : c + 1, :], -2)
        match = (column == used.astype(jnp.float32)).astype(jnp.float32)
        weights_ref[c] = lax.dot_general(
            coef_ref[c],
            match,
            (((0,), (1,)), ((), ())),
            preferred_element_type=jnp.float32,
            precision=HIGHEST,
        )

    for kb, kd in peers:
        sb, sd = target(kb, kd)
        arrived(sb * dirs + sd, rays_all, ray_recv)

    group = 4 if top_local % 4 == 0 else 1

    def far_group(g, carry):
        base = g * group
        weight = [weights_ref[base + i] for i in range(group)]
        total = [jnp.zeros((rows, samples), jnp.float32) for _ in range(group)]
        for slot in range(boxes * dirs):
            for j in range(runs):
                ray = rays_all[slot, j].astype(jnp.float32)
                at = slot * runs + j
                for i in range(group):
                    total[i] = total[i] + weight[i][:, at : at + 1] * ray
        for i in range(group):
            far_ref[base + i] = total[i]
        return carry

    lax.fori_loop(0, top_local // group, far_group, 0)

    incoming = jnp.dot(
        far_ref[...].reshape(top_local * rows, samples),
        time_matrix,
        preferred_element_type=jnp.float32,
        precision=HIGHEST,
    )
    far_ref[...] = incoming.reshape(top_local, rows, samples)
    first_top = my_box * top_local
    for d in range(dirs):
        held = parent_all[my_box * dirs + d]
        for j in range(runs):
            at = (my_box * dirs + d) * runs + j
            parent = jnp.sum(jnp.where(lane == at, held, 0.0), axis=1, keepdims=True)
            chosen = jnp.zeros((rows, samples), jnp.float32)
            for c in range(top_local):
                hit = parent == (first_top + c).astype(jnp.float32)
                chosen = jnp.where(hit, far_ref[c], chosen)
            stage_ref[d, j] = chosen.astype(jnp.bfloat16)

    def back_copy(kd):
        td = lax.rem(my_dir + kd, dirs)
        return pltpu.make_async_remote_copy(
            src_ref=stage_ref.at[td],
            dst_ref=landed.at[my_dir],
            send_sem=back_send.at[td],
            recv_sem=back_recv.at[my_dir],
            device_id={"box": my_box, "dir": td},
            device_id_type=MESH,
        )

    for kd in range(1, dirs):
        back_copy(kd).start()
    landed[my_dir] = stage_ref[my_dir]
    for kb, kd in peers:
        parent_copy(kb, kd).wait_send()
        ray_copy(kb, kd).wait_send()

    @pl.when(me < devices - 1)
    def _():
        rim_copy(0).wait_send()
        rim_copy(1).wait_recv()

    @pl.when(me > 0)
    def _():
        rim_copy(1).wait_send()
        rim_copy(0).wait_recv()

    rim_ref[...] = rim[...]
    for kd in range(1, dirs):
        sd = lax.rem(my_dir + kd, dirs)
        arrived(sd, landed, back_recv)
    for d in range(dirs):
        for j in range(runs):
            out_ref[d * rows : (d + 1) * rows, j * samples : (j + 1) * samples] = landed[d, j]
    for kd in range(1, dirs):
        back_copy(kd).wait_send()


def field_kernel(
    runs, chunk, blocks_ref, maps_ref, incoming_ref, links_ref, cur_ref, rim_ref, out_ref
):
    step = pl.program_id(0)
    samples = cur_ref.shape[-1]
    first = step * chunk
    dot = functools.partial(jnp.dot, preferred_element_type=jnp.float32)

    def joined(parts):
        return jnp.concatenate(parts, axis=1)

    before = jnp.maximum(first - 1, 0)
    after = jnp.minimum(first + chunk, LEAF_TOP - 1)
    final = step == pl.num_programs(0) - 1
    lead = [rim_ref[0]] + [cur_ref[j, LEAF_TOP - 1] for j in range(runs - 1)]
    tail = [cur_ref[j, 0] for j in range(1, runs)] + [rim_ref[1]]
    lead = [jnp.where(step == 0, lead[j], cur_ref[j, before]) for j in range(runs)]
    tail = [jnp.where(final, tail[j], cur_ref[j, after]) for j in range(runs)]
    pairs = [joined(lead)]
    pairs += [joined([cur_ref[j, first + i] for j in range(runs)]) for i in range(chunk)]
    pairs += [joined(tail)]
    for i in range(chunk):
        at = first + i
        total = dot(blocks_ref[0], pairs[i + 1]) + dot(maps_ref[at], incoming_ref[...])
        low = dot(blocks_ref[1], pairs[i])
        high = dot(blocks_ref[2], pairs[i + 2])
        for j in range(runs):
            span = slice(j * samples, (j + 1) * samples)
            with_low = links_ref[0, j * LEAF_TOP + at].astype(jnp.float32)
            with_high = links_ref[1, j * LEAF_TOP + at].astype(jnp.float32)
            part = total[:, span] + with_low * low[:, span] + with_high * high[:, span]
            out_ref[j, i] = part.astype(jnp.bfloat16)


def per_device(
    currents,
    leaf_parent,
    near_links,
    near_blocks,
    aggregate_maps,
    far_boxes,
    far_counts,
    translate_coef,
    time_kernel,
    disaggregate_maps,
):
    boxes, dirs = lax.axis_size("box"), lax.axis_size("dir")
    devices = boxes * dirs
    leaf_count, unknowns, samples = currents.shape
    runs = leaf_count // LEAF_TOP
    top_local, list_slots = far_boxes.shape
    directions = aggregate_maps.shape[1]
    rows = directions // dirs
    dir_index = lax.axis_index("dir")
    f32, bf16 = jnp.float32, jnp.bfloat16

    leaf_runs = currents.reshape(runs, LEAF_TOP, unknowns, samples)

    chunk = 8
    steps = LEAF_TOP // chunk
    matmul_cost = 2 * leaf_count * samples * unknowns * directions
    vmem = pl.BlockSpec(memory_space=pltpu.VMEM)
    rays = pl.pallas_call(
        functools.partial(aggregate_kernel, runs, chunk),
        out_shape=jax.ShapeDtypeStruct((runs, directions, samples), bf16),
        grid=(steps,),
        in_specs=[
            pl.BlockSpec((chunk, directions, unknowns), lambda i: (i, 0, 0)),
            pl.BlockSpec((runs, chunk, unknowns, samples), lambda i: (0, i, 0, 0)),
        ],
        out_specs=pl.BlockSpec((runs, directions, samples), lambda i: (0, 0, 0)),
        scratch_shapes=[pltpu.VMEM((directions, runs * samples), f32)],
        cost_estimate=pl.CostEstimate(
            flops=matmul_cost, bytes_accessed=16 * 2**20, transcendentals=0
        ),
        name="aggregate",
    )(aggregate_maps, leaf_runs)

    total_runs = devices * runs
    width = -(-total_runs // 128) * 128
    coef = lax.dynamic_slice_in_dim(translate_coef, dir_index * rows, rows, 2)
    edges = jnp.stack([currents[-1], currents[0]])
    smem = pl.BlockSpec(memory_space=pltpu.SMEM)
    dma = pltpu.SemaphoreType.DMA
    incoming, rim = pl.pallas_call(
        functools.partial(translate_kernel, boxes, dirs, runs, top_local),
        out_shape=(
            jax.ShapeDtypeStruct((directions, runs * samples), bf16),
            jax.ShapeDtypeStruct((2, unknowns, samples), bf16),
        ),
        in_specs=[vmem, vmem, smem, vmem, smem, vmem, smem],
        out_specs=(vmem, vmem),
        scratch_shapes=[
            pltpu.VMEM((1, width), f32),
            pltpu.VMEM((2, unknowns, samples), bf16),
            pltpu.VMEM((devices, runs, rows, samples), bf16),
            pltpu.VMEM((devices, 1, width), f32),
            pltpu.VMEM((top_local, rows, width), f32),
            pltpu.VMEM((top_local, rows, samples), f32),
            pltpu.VMEM((dirs, runs, rows, samples), bf16),
            pltpu.VMEM((dirs, runs, rows, samples), bf16),
            dma((devices,)),
            dma((devices,)),
            dma((devices,)),
            dma((devices,)),
            dma((dirs,)),
            dma((dirs,)),
            dma((2,)),
            dma((2,)),
        ],
        compiler_params=pltpu.CompilerParams(
            collective_id=0, has_side_effects=True, vmem_limit_bytes=16 * 2**20
        ),
        cost_estimate=pl.CostEstimate(
            flops=8 * matmul_cost, bytes_accessed=2 * 2**20, transcendentals=0
        ),
        name="translate",
    )(rays, edges, leaf_parent, far_boxes, far_counts, coef, time_kernel)

    near_cost = 4 * matmul_cost
    out = pl.pallas_call(
        functools.partial(field_kernel, runs, chunk),
        out_shape=jax.ShapeDtypeStruct((runs, LEAF_TOP, unknowns, samples), bf16),
        grid=(steps,),
        in_specs=[vmem, vmem, vmem, smem, vmem, vmem],
        out_specs=pl.BlockSpec((runs, chunk, unknowns, samples), lambda i: (0, i, 0, 0)),
        cost_estimate=pl.CostEstimate(
            flops=near_cost, bytes_accessed=26 * 2**20, transcendentals=0
        ),
        name="field",
        compiler_params=pltpu.CompilerParams(vmem_limit_bytes=12 * 2**20),
    )(near_blocks, disaggregate_maps, incoming, near_links.T, leaf_runs, rim)
    return out.reshape(leaf_count, unknowns, samples)


def solution(mesh):
    return jax.shard_map(
        per_device,
        mesh=mesh,
        in_specs=(
            P(("box", "dir"), None, None),
            P(("box", "dir")),
            P(("box", "dir"), None),
            P(),
            P(),
            P("box", None),
            P("box"),
            P("box", None, None),
            P(),
            P(),
        ),
        out_specs=P(("box", "dir"), None, None),
        check_vma=False,
    )
```

```python
import functools
import jax
import jax.numpy as jnp
from jax import lax
from jax.experimental import pallas as pl
from jax.experimental.pallas import tpu as pltpu
from jax.sharding import PartitionSpec as P

LEAF_TOP = 64
MESH = pl.DeviceIdType.MESH
HIGHEST = lax.Precision.HIGHEST


def aggregate_kernel(runs, chunk, maps_ref, cur_ref, out_ref, edge_ref, acc_ref):
    step = pl.program_id(0)
    samples = cur_ref.shape[-1]

    @pl.when(step == 0)
    def _():
        acc_ref[...] = jnp.zeros_like(acc_ref)
        edge_ref[1] = cur_ref[0, 0]

    maps = jnp.concatenate([maps_ref[i] for i in range(chunk)], axis=1)
    depth = chunk * cur_ref.shape[2]
    leaves = jnp.concatenate([cur_ref[j].reshape(depth, samples) for j in range(runs)], axis=1)
    acc_ref[...] += jnp.dot(maps, leaves, preferred_element_type=jnp.float32)

    @pl.when(step == pl.num_programs(0) - 1)
    def _():
        edge_ref[0] = cur_ref[runs - 1, chunk - 1]
        for j in range(runs):
            out_ref[j] = acc_ref[:, j * samples : (j + 1) * samples].astype(jnp.bfloat16)


def translate_kernel(
    boxes,
    dirs,
    runs,
    top_local,
    rays_ref,
    edge_ref,
    leaf_parent_ref,
    lists_ref,
    counts_ref,
    coef_ref,
    kernel_ref,
    out_ref,
    rim_ref,
    parent_ref,
    rim,
    rays_all,
    parent_all,
    weights_ref,
    far_ref,
    stage_ref,
    landed,
    ray_send,
    ray_recv,
    par_send,
    par_recv,
    back_send,
    back_recv,
    rim_send,
    rim_recv,
):
    my_box = lax.axis_index("box")
    my_dir = lax.axis_index("dir")
    me = my_box * dirs + my_dir
    devices = boxes * dirs
    rows = coef_ref.shape[2]
    samples = rays_ref.shape[-1]
    width = parent_ref.shape[-1]
    lane = lax.broadcasted_iota(jnp.int32, (1, width), 1)
    spare = jnp.where(me == 0, -1, 0)
    parent_row = jnp.where(lane >= devices * runs, spare, jnp.zeros((1, width), jnp.int32))
    for j in range(runs):
        parent_row = jnp.where(lane == me * runs + j, leaf_parent_ref[j * LEAF_TOP], parent_row)
    parent_ref[...] = parent_row.astype(jnp.float32)
    rim[...] = jnp.zeros_like(rim)
    peers = [(kb, kd) for kb in range(boxes) for kd in range(dirs) if kb or kd]
    peers.sort(key=lambda p: -min(p[0], boxes - p[0]))

    def target(kb, kd):
        return lax.rem(my_box + kb, boxes), lax.rem(my_dir + kd, dirs)

    barrier = pltpu.get_barrier_semaphore()
    for kb, kd in peers:
        tb, td = target(kb, kd)
        pl.semaphore_signal(
            barrier, inc=1, device_id={"box": tb, "dir": td}, device_id_type=MESH
        )
    pl.semaphore_wait(barrier, len(peers))

    def parent_copy(kb, kd):
        tb, td = target(kb, kd)
        return pltpu.make_async_remote_copy(
            src_ref=parent_ref,
            dst_ref=parent_all.at[me],
            send_sem=par_send.at[tb * dirs + td],
            recv_sem=par_recv.at[me],
            device_id={"box": tb, "dir": td},
            device_id_type=MESH,
        )

    def ray_copy(kb, kd):
        tb, td = target(kb, kd)
        block = pl.ds(pl.multiple_of(td * rows, rows), rows)
        return pltpu.make_async_remote_copy(
            src_ref=rays_ref.at[:, block, :],
            dst_ref=rays_all.at[me],
            send_sem=ray_send.at[tb * dirs + td],
            recv_sem=ray_recv.at[me],
            device_id={"box": tb, "dir": td},
            device_id_type=MESH,
        )

    def rim_copy(side):
        other = lax.rem(me + (1 if side == 0 else devices - 1), devices)
        return pltpu.make_async_remote_copy(
            src_ref=edge_ref.at[side],
            dst_ref=rim.at[side],
            send_sem=rim_send.at[side],
            recv_sem=rim_recv.at[side],
            device_id={"box": lax.div(other, dirs), "dir": lax.rem(other, dirs)},
            device_id_type=MESH,
        )

    for kb, kd in peers:
        parent_copy(kb, kd).start()
    for kb, kd in peers:
        ray_copy(kb, kd).start()

    @pl.when(me < devices - 1)
    def _():
        rim_copy(0).start()

    @pl.when(me > 0)
    def _():
        rim_copy(1).start()

    own = pl.ds(pl.multiple_of(my_dir * rows, rows), rows)
    rays_all[me] = rays_ref[:, own, :]
    parent_all[me] = parent_ref[...]

    lag = lax.broadcasted_iota(jnp.int32, (samples, samples), 1) - lax.broadcasted_iota(
        jnp.int32, (samples, samples), 0
    )

    def add_lag(i, matrix):
        return jnp.where(lag == i, kernel_ref[i], matrix)

    time_matrix = lax.fori_loop(
        0, samples, add_lag, jnp.zeros((samples, samples), jnp.float32)
    )

    def arrived(slot, buffer, sem):
        pltpu.make_async_remote_copy(
            src_ref=buffer.at[slot],
            dst_ref=buffer.at[slot],
            send_sem=sem.at[slot],
            recv_sem=sem.at[slot],
            device_id={"box": my_box, "dir": lax.rem(my_dir + 1, dirs)},
            device_id_type=MESH,
        ).wait_recv()

    for kb, kd in peers:
        sb, sd = target(kb, kd)
        arrived(sb * dirs + sd, parent_all, par_recv)
    parents = jnp.zeros((1, width), jnp.float32)
    for slot in range(devices):
        parents = parents + parent_all[slot]
    slots = lists_ref.shape[1]
    column = jnp.broadcast_to(parents, (128, width)).T[:, :slots]
    spot = lax.broadcasted_iota(jnp.int32, (1, slots), 1)
    for c in range(top_local):
        used = jnp.where(spot < counts_ref[c], lists_ref[c : c + 1, :], -2)
        match = (column == used.astype(jnp.float32)).astype(jnp.float32)
        weights_ref[c] = lax.dot_general(
            coef_ref[c],
            match,
            (((0,), (1,)), ((), ())),
            preferred_element_type=jnp.float32,
            precision=HIGHEST,
        )

    for kb, kd in peers:
        sb, sd = target(kb, kd)
        arrived(sb * dirs + sd, rays_all, ray_recv)

    group = 4 if top_local % 4 == 0 else 1

    def far_group(g, carry):
        base = g * group
        weight = [weights_ref[base + i] for i in range(group)]
        total = [jnp.zeros((rows, samples), jnp.float32) for _ in range(group)]
        for slot in range(boxes * dirs):
            for j in range(runs):
                ray = rays_all[slot, j].astype(jnp.float32)
                at = slot * runs + j
                for i in range(group):
                    total[i] = total[i] + weight[i][:, at : at + 1] * ray
        for i in range(group):
            far_ref[base + i] = total[i]
        return carry

    lax.fori_loop(0, top_local // group, far_group, 0)

    incoming = jnp.dot(
        far_ref[...].reshape(top_local * rows, samples),
        time_matrix,
        preferred_element_type=jnp.float32,
        precision=HIGHEST,
    )
    far_ref[...] = incoming.reshape(top_local, rows, samples)
    first_top = my_box * top_local
    for d in range(dirs):
        held = parent_all[my_box * dirs + d]
        for j in range(runs):
            at = (my_box * dirs + d) * runs + j
            parent = jnp.sum(jnp.where(lane == at, held, 0.0), axis=1, keepdims=True)
            chosen = jnp.zeros((rows, samples), jnp.float32)
            for c in range(top_local):
                hit = parent == (first_top + c).astype(jnp.float32)
                chosen = jnp.where(hit, far_ref[c], chosen)
            stage_ref[d, j] = chosen.astype(jnp.bfloat16)

    def back_copy(kd):
        td = lax.rem(my_dir + kd, dirs)
        return pltpu.make_async_remote_copy(
            src_ref=stage_ref.at[td],
            dst_ref=landed.at[my_dir],
            send_sem=back_send.at[td],
            recv_sem=back_recv.at[my_dir],
            device_id={"box": my_box, "dir": td},
            device_id_type=MESH,
        )

    for kd in range(1, dirs):
        back_copy(kd).start()
    landed[my_dir] = stage_ref[my_dir]
    for kb, kd in peers:
        parent_copy(kb, kd).wait_send()
        ray_copy(kb, kd).wait_send()

    @pl.when(me < devices - 1)
    def _():
        rim_copy(0).wait_send()
        rim_copy(1).wait_recv()

    @pl.when(me > 0)
    def _():
        rim_copy(1).wait_send()
        rim_copy(0).wait_recv()

    rim_ref[...] = rim[...]
    for kd in range(1, dirs):
        sd = lax.rem(my_dir + kd, dirs)
        arrived(sd, landed, back_recv)
    for d in range(dirs):
        for j in range(runs):
            out_ref[d * rows : (d + 1) * rows, j * samples : (j + 1) * samples] = landed[d, j]
    for kd in range(1, dirs):
        back_copy(kd).wait_send()


def field_kernel(
    runs, chunk, blocks_ref, maps_ref, incoming_ref, links_ref, cur_ref, rim_ref, out_ref
):
    step = pl.program_id(0)
    samples = cur_ref.shape[-1]
    first = step * chunk
    dot = functools.partial(jnp.dot, preferred_element_type=jnp.float32)

    def joined(parts):
        return jnp.concatenate(parts, axis=1)

    before = jnp.maximum(first - 1, 0)
    after = jnp.minimum(first + chunk, LEAF_TOP - 1)
    final = step == pl.num_programs(0) - 1
    lead = [rim_ref[0]] + [cur_ref[j, LEAF_TOP - 1] for j in range(runs - 1)]
    tail = [cur_ref[j, 0] for j in range(1, runs)] + [rim_ref[1]]
    lead = [jnp.where(step == 0, lead[j], cur_ref[j, before]) for j in range(runs)]
    tail = [jnp.where(final, tail[j], cur_ref[j, after]) for j in range(runs)]
    spans = [slice(j * samples, (j + 1) * samples) for j in range(runs)]
    pairs = [joined(lead)]
    pairs += [joined([cur_ref[j, first + i] for j in range(runs)]) for i in range(chunk)]
    pairs += [joined(tail)]
    for i in range(chunk):
        at = first + i
        low = [pairs[i][:, span] for span in spans]
        high = [pairs[i + 2][:, span] for span in spans]
        for j in range(runs):
            leaf = j * LEAF_TOP + at
            low[j] = jnp.where(links_ref[0, leaf] != 0, low[j], jnp.zeros_like(low[j]))
            high[j] = jnp.where(links_ref[1, leaf] != 0, high[j], jnp.zeros_like(high[j]))
        left = joined([blocks_ref[0], blocks_ref[1], blocks_ref[2], maps_ref[at]])
        right = [pairs[i + 1], joined(low), joined(high), incoming_ref[...]]
        total = dot(left, jnp.concatenate(right, axis=0))
        for j in range(runs):
            out_ref[j, i] = total[:, spans[j]].astype(jnp.bfloat16)


def per_device(
    currents,
    leaf_parent,
    near_links,
    near_blocks,
    aggregate_maps,
    far_boxes,
    far_counts,
    translate_coef,
    time_kernel,
    disaggregate_maps,
):
    boxes, dirs = lax.axis_size("box"), lax.axis_size("dir")
    devices = boxes * dirs
    leaf_count, unknowns, samples = currents.shape
    runs = leaf_count // LEAF_TOP
    top_local, list_slots = far_boxes.shape
    directions = aggregate_maps.shape[1]
    rows = directions // dirs
    dir_index = lax.axis_index("dir")
    f32, bf16 = jnp.float32, jnp.bfloat16

    leaf_runs = currents.reshape(runs, LEAF_TOP, unknowns, samples)

    chunk = 8
    steps = LEAF_TOP // chunk
    matmul_cost = 2 * leaf_count * samples * unknowns * directions
    vmem = pl.BlockSpec(memory_space=pltpu.VMEM)
    rays, edges = pl.pallas_call(
        functools.partial(aggregate_kernel, runs, chunk),
        out_shape=(
            jax.ShapeDtypeStruct((runs, directions, samples), bf16),
            jax.ShapeDtypeStruct((2, unknowns, samples), bf16),
        ),
        grid=(steps,),
        in_specs=[
            pl.BlockSpec((chunk, directions, unknowns), lambda i: (i, 0, 0)),
            pl.BlockSpec((runs, chunk, unknowns, samples), lambda i: (0, i, 0, 0)),
        ],
        out_specs=(
            pl.BlockSpec((runs, directions, samples), lambda i: (0, 0, 0)),
            pl.BlockSpec((2, unknowns, samples), lambda i: (0, 0, 0)),
        ),
        compiler_params=pltpu.CompilerParams(vmem_limit_bytes=58 * 2**20),
        scratch_shapes=[pltpu.VMEM((directions, runs * samples), f32)],
        cost_estimate=pl.CostEstimate(
            flops=matmul_cost, bytes_accessed=16 * 2**20, transcendentals=0
        ),
        name="aggregate",
    )(aggregate_maps, leaf_runs)

    total_runs = devices * runs
    width = -(-total_runs // 128) * 128
    coef = lax.dynamic_slice_in_dim(translate_coef, dir_index * rows, rows, 2)
    smem = pl.BlockSpec(memory_space=pltpu.SMEM)
    dma = pltpu.SemaphoreType.DMA
    incoming, rim = pl.pallas_call(
        functools.partial(translate_kernel, boxes, dirs, runs, top_local),
        out_shape=(
            jax.ShapeDtypeStruct((directions, runs * samples), bf16),
            jax.ShapeDtypeStruct((2, unknowns, samples), bf16),
        ),
        in_specs=[vmem, pl.BlockSpec(memory_space=pl.ANY), smem, vmem, smem, vmem, smem],
        out_specs=(vmem, vmem),
        scratch_shapes=[
            pltpu.VMEM((1, width), f32),
            pltpu.VMEM((2, unknowns, samples), bf16),
            pltpu.VMEM((devices, runs, rows, samples), bf16),
            pltpu.VMEM((devices, 1, width), f32),
            pltpu.VMEM((top_local, rows, width), f32),
            pltpu.VMEM((top_local, rows, samples), f32),
            pltpu.VMEM((dirs, runs, rows, samples), bf16),
            pltpu.VMEM((dirs, runs, rows, samples), bf16),
            dma((devices,)),
            dma((devices,)),
            dma((devices,)),
            dma((devices,)),
            dma((dirs,)),
            dma((dirs,)),
            dma((2,)),
            dma((2,)),
        ],
        compiler_params=pltpu.CompilerParams(
            collective_id=0, has_side_effects=True, vmem_limit_bytes=16 * 2**20
        ),
        cost_estimate=pl.CostEstimate(
            flops=8 * matmul_cost, bytes_accessed=2 * 2**20, transcendentals=0
        ),
        name="translate",
    )(rays, edges, leaf_parent, far_boxes, far_counts, coef, time_kernel)

    near_cost = 4 * matmul_cost
    out = pl.pallas_call(
        functools.partial(field_kernel, runs, chunk),
        out_shape=jax.ShapeDtypeStruct((runs, LEAF_TOP, unknowns, samples), bf16),
        grid=(steps,),
        in_specs=[vmem, vmem, vmem, smem, vmem, vmem],
        out_specs=pl.BlockSpec((runs, chunk, unknowns, samples), lambda i: (0, i, 0, 0)),
        cost_estimate=pl.CostEstimate(
            flops=near_cost, bytes_accessed=26 * 2**20, transcendentals=0
        ),
        name="field",
        compiler_params=pltpu.CompilerParams(vmem_limit_bytes=12 * 2**20),
    )(near_blocks, disaggregate_maps, incoming, near_links.T, leaf_runs, rim)
    return out.reshape(leaf_count, unknowns, samples)


def solution(mesh):
    return jax.shard_map(
        per_device,
        mesh=mesh,
        in_specs=(
            P(("box", "dir"), None, None),
            P(("box", "dir")),
            P(("box", "dir"), None),
            P(),
            P(),
            P("box", None),
            P("box"),
            P("box", None, None),
            P(),
            P(),
        ),
        out_specs=P(("box", "dir"), None, None),
        check_vma=False,
    )
```
